32 devices in a mesh: freq: 8 (over z, x), pts: 4 (over y, core).
Axes of the slice: x: 2, y: 2, z: 4, core: 2. Of those that a mesh axis runs over, the one named last changes fastest.
Arguments:
- snapshots: float32 [256, 5, 8192], P(None, None, ('pts', 'freq')), may hold values from -6 to 6
- weights: float32 [8192], P(('pts', 'freq')), may hold values from 0.25 to 4
- starts: int32 [3], replicated, may hold values from 0 to 128
- bins: int32 [64], replicated, may hold values from 0 to 63, each once
Outputs:
- modes: float32 [64, 2, 5, 8192], P('freq', None, None, 'pts')
- energy: float32 [64], P('freq')
The draws below stay inside these ranges and needn't reach their ends.
All inputs are finite; a program needn't handle non-finite values.
Results may differ from the reference program's by a relative error of at most 0.00024.
Values sent between devices are 32-bit elements; how exact they have to be, the bound alone decides.
A program may use at most 64 MiB of HBM per device.

```python
import math
import jax
import jax.numpy as jnp
from jax import lax

NVAR = 5
NFFT = 128
NB = 3
ITERS = 8
KF = 64
NT = 256
NPTS = 8192


def block_scale(stream_key, dims, shards, least, largest):
    def one(dim, shards_of):
        steps = jax.random.uniform(jax.random.fold_in(jax.random.fold_in(stream_key, 6), dim), (shards_of,), jnp.float32, least / len(shards), largest / len(shards))
        return jnp.repeat(jnp.exp(steps), dims[dim] // shards_of).reshape((-1,) + (1,) * (len(dims) - dim - 1))

    loudness = one(*shards[0])
    for cut in shards[1:]:
        loudness = loudness * one(*cut)
    return loudness


def noise(stream_key, dims, deviation, limit, shards=(), kind=jnp.bfloat16):
    drawn = jax.random.normal(stream_key, dims, jnp.float32) * deviation
    if len(shards) > 0:
        drawn = block_scale(stream_key, dims, shards, -0.22, 0.18) * drawn
    return jnp.clip(drawn, min=-limit, max=limit).astype(kind)


def setup_inputs(seed: int = 0) -> dict:
    seeds = jax.random.split(jax.random.key(seed), 5)
    return {
        "snapshots": noise(seeds[0], (NT, NVAR, NPTS), 1.0, 6.0, ((2, 32),), jnp.float32),
        "weights": jnp.clip(jnp.exp(math.log(4.0) - 2.7725887 * jax.random.uniform(seeds[1], (NPTS,), jnp.float32) ** block_scale(seeds[1], (NPTS,), ((0, 32),), -0.2, 0.2)), 0.25, 4.0),
        "starts": jax.random.randint(seeds[2], (NB,), 0, NT - NFFT + 1).astype(jnp.int32),
        "bins": jax.random.permutation(seeds[3], KF).astype(jnp.int32),
    }


def dft_window():
    steps_t = jnp.arange(NFFT, dtype=jnp.float32)
    window = 0.5 - 0.5 * jnp.cos(2.0 * math.pi * steps_t / NFFT)
    return (window, 1.0 / jnp.sqrt(jnp.sum(window * window)))

def gram_of(spec, wts, count):
    weighted = spec * wts
    real_part = jnp.einsum('kacvp,kbcvp->kab', weighted, spec, precision=lax.Precision.HIGHEST)
    cross = jnp.einsum('kavp,kbvp->kab', weighted[:, :, 0], spec[:, :, 1], precision=lax.Precision.HIGHEST)
    return (real_part / count, (cross - jnp.swapaxes(cross, 1, 2)) / count)

def apply_gram(gram_re, gram_im, xr, xi):
    ur = lax.optimization_barrier(jnp.sum(gram_re * xr[:, None, :], 2)) - lax.optimization_barrier(jnp.sum(gram_im * xi[:, None, :], 2))
    ui = lax.optimization_barrier(jnp.sum(gram_re * xi[:, None, :], 2)) + lax.optimization_barrier(jnp.sum(gram_im * xr[:, None, :], 2))
    return (ur, ui)

def leading(gram_re, gram_im):
    xr = jnp.ones(gram_re.shape[:2], gram_re.dtype)
    xi = jnp.zeros(gram_re.shape[:2], gram_re.dtype)
    for step in range(ITERS):
        ur, ui = apply_gram(gram_re, gram_im, xr, xi)
        scale_now = jnp.sqrt(lax.optimization_barrier(jnp.sum(ur * ur + ui * ui, 1)))[:, None]
        xr, xi = (ur / scale_now, ui / scale_now)
    ur, ui = apply_gram(gram_re, gram_im, xr, xi)
    return (xr, xi, lax.optimization_barrier(jnp.sum(xr * ur + xi * ui, 1)))

def build_modes(spec, xr, xi, energy):
    hp = lax.Precision.HIGHEST
    real_part = jnp.einsum('kb,kbvp->kvp', xr, spec[:, :, 0], precision=hp) - jnp.einsum('kb,kbvp->kvp', xi, spec[:, :, 1], precision=hp)
    imag_part = jnp.einsum('kb,kbvp->kvp', xr, spec[:, :, 1], precision=hp) + jnp.einsum('kb,kbvp->kvp', xi, spec[:, :, 0], precision=hp)
    factor = 1.0 / jnp.sqrt(jnp.maximum(energy, 0.25))
    return jnp.stack([real_part, imag_part], 1) * factor[:, None, None, None]

def reference(snapshots, weights, starts, bins):
    centered = snapshots - lax.optimization_barrier(jnp.mean(snapshots, 0, keepdims=True))
    window, scale = dft_window()
    blocks = []
    for block in range(NB):
        segment = lax.dynamic_slice_in_dim(centered, starts[block].astype(jnp.int32), NFFT, 0)
        transformed = jnp.fft.rfft(segment * window[:, None, None], axis=0)[bins.astype(jnp.int32)]
        blocks.append(jnp.stack([jnp.real(transformed), jnp.imag(transformed)], 1) * scale)
    spec = jnp.stack(blocks, 1)
    gram_re, gram_im = gram_of(spec, weights, NPTS * NVAR)
    xr, xi, energy = leading(gram_re, gram_im)
    return (build_modes(spec, xr, xi, energy), energy)
```

```python
import functools
import math

import jax
import jax.numpy as jnp
import numpy as np
from jax import lax
from jax.experimental import pallas as pl
from jax.experimental.pallas import tpu as pltpu
from jax.sharding import PartitionSpec as P

NFFT = 128
ITERS = 8
LANES = 128
SUB = 8
MESH = pl.DeviceIdType.MESH


def base_table(nfft):
    steps = np.arange(nfft)
    window = 0.5 - 0.5 * np.cos(2.0 * math.pi * steps / nfft)
    scale = 1.0 / np.sqrt(np.sum(window * window))
    phase = (np.arange(nfft // 2)[:, None] * steps[None, :] % nfft) * (2.0 * math.pi / nfft)
    return np.concatenate([np.cos(phase) * scale, -np.sin(phase) * scale], 1).astype(np.float32)


def window_table(nfft, n_time):
    rel = np.arange(n_time)[None, :] - np.arange(n_time - nfft + 1)[:, None]
    window = 0.5 - 0.5 * np.cos(2.0 * math.pi * rel / nfft)
    return np.where((rel >= 0) & (rel < nfft), window, 0.0).astype(np.float32)


def split(x):
    hi = x.astype(jnp.bfloat16)
    lo = (x - hi.astype(jnp.float32)).astype(jnp.bfloat16)
    return hi, lo


def pick_rows(rows, shape):
    index = lax.broadcasted_iota(jnp.int32, shape, 0)
    out = jnp.zeros(shape, rows[0].dtype)
    for r, value in enumerate(rows):
        out = jnp.where(index == r, value, out)
    return out


def kernel(
    n_freq, n_pts, n_blocks, count, snap_hbm, w_hbm, starts_hbm, bins_1d, bins_hbm, base_hbm, window_hbm,
    recv_ref, energy_ref,
    snap, w_ref, bins_ref, base_ref, window_ref, tab, tab3, spec, gacc, gsend1, grecv1, gsend2, grecv2, coef, send, laid,
    starts_ref, bins_smem, load_sem, small_sem, s1, r1, s2, r2, s3, r3, own_sem,
):
    n_var, n_time, n_local = snap.shape
    n_bins = bins_smem.shape[0]
    per = n_bins // n_freq
    tiles = n_local // LANES
    step = n_var * tiles * 2
    fr = lax.axis_index("freq")
    pt = lax.axis_index("pts")

    small = [
        pltpu.make_async_copy(src, dst, small_sem.at[i])
        for i, (src, dst) in enumerate(
            [
                (bins_1d, bins_smem), (starts_hbm, starts_ref), (base_hbm, base_ref), (window_hbm, window_ref),
                (w_hbm, w_ref), (bins_hbm, bins_ref),
            ]
        )
    ]
    for copy in small:
        copy.start()
    for v in range(n_var):
        pltpu.make_async_copy(snap_hbm.at[v], snap.at[v], load_sem.at[v]).start()

    barrier = pltpu.get_barrier_semaphore()
    for d in range(1, n_pts):
        pl.semaphore_signal(barrier, inc=1, device_id={"pts": lax.rem(pt + d, n_pts)}, device_id_type=MESH)
    for d in range(1, n_freq):
        pl.semaphore_signal(barrier, inc=1, device_id={"freq": lax.rem(fr + d, n_freq)}, device_id_type=MESH)

    for copy in small:
        copy.wait()
    for j in range(n_bins):
        tab[pl.ds(j, 1), :] = base_ref[pl.ds(bins_smem[j], 1), :]
    starts = [starts_ref[b] for b in range(n_blocks)]
    cs = tab[:, :NFFT]
    sn = tab[:, NFFT:]
    reps = n_time // NFFT
    full = jnp.concatenate([jnp.concatenate([cs] * reps, 1), jnp.concatenate([sn] * reps, 1)], 0)
    for b in range(n_blocks):
        hi, lo = split(full * window_ref[pl.ds(starts[b], 1), :])
        rows = pl.ds(b * 2 * n_bins, 2 * n_bins)
        tab3[rows, 0:n_time] = hi
        tab3[rows, n_time : 2 * n_time] = lo
        tab3[rows, 2 * n_time : 3 * n_time] = hi

    wts = [jnp.broadcast_to(w_ref[:, l * LANES : (l + 1) * LANES], (SUB, LANES)) for l in range(tiles)]
    pairs = [(a, c) for a in range(n_blocks) for c in range(a + 1, n_blocks)]
    n_entries = n_blocks * n_blocks

    if n_entries % 2:
        gacc[n_entries * n_bins :, :] = jnp.zeros((n_bins, LANES), jnp.float32)
    for v in range(n_var):
        pltpu.make_async_copy(snap_hbm.at[v], snap.at[v], load_sem.at[v]).wait()
        x = snap[v]
        x = x - jnp.sum(x, 0, keepdims=True) * (1.0 / n_time)
        hi, lo = split(x)
        x3 = jnp.concatenate([hi, hi, lo], 0)
        spec[:, v * n_local : (v + 1) * n_local] = jnp.dot(
            tab3[...], x3, preferred_element_type=jnp.float32
        )
        for g in range(n_bins // SUB):
            total = [None] * n_entries
            for l in range(tiles):
                lane = slice((v * tiles + l) * LANES, (v * tiles + l + 1) * LANES)
                part = [
                    [spec[pl.ds((b * 2 + c) * n_bins + g * SUB, SUB), lane] for c in range(2)]
                    for b in range(n_blocks)
                ]
                wp = [[part[b][c] * wts[l] for c in range(2)] for b in range(n_blocks)]
                new = [wp[b][0] * part[b][0] + wp[b][1] * part[b][1] for b in range(n_blocks)]
                for a, c in pairs:
                    new.append(wp[a][0] * part[c][0] + wp[a][1] * part[c][1])
                    new.append(wp[a][0] * part[c][1] - wp[a][1] * part[c][0])
                total = [n if t is None else t + n for t, n in zip(total, new)]
            for e in range(n_entries):
                rows = pl.ds(e * n_bins + g * SUB, SUB)
                gacc[rows, :] = total[e] if v == 0 else gacc[rows, :] + total[e]

    ones = jnp.ones((SUB, 2 * LANES), jnp.bfloat16)
    rows = []
    for p in range((n_entries + 1) // 2):
        hi, lo = split(gacc[pl.ds(p * 2 * n_bins, 2 * n_bins), :])
        rows.append(
            lax.dot_general(
                ones, jnp.concatenate([hi, lo], 1), (((1,), (1,)), ((), ())),
                preferred_element_type=jnp.float32,
            )
        )
    mine = pick_rows(rows, (SUB, 2 * n_bins))[: len(rows)]
    gsend1[...] = mine
    grecv1[pt] = mine

    pl.semaphore_wait(barrier, n_pts + n_freq - 2)

    def exchange(axis, me, n, src, dst, send_sems, recv_sems, meanwhile=lambda: None):
        copies = []
        for d in range(1, n):
            copy = pltpu.make_async_remote_copy(
                src_ref=src, dst_ref=dst.at[me], send_sem=send_sems.at[d - 1], recv_sem=recv_sems.at[me],
                device_id={axis: lax.rem(me + d, n)}, device_id_type=MESH,
            )
            copy.start()
            copies.append(copy)
        done = meanwhile()
        for d in range(1, n):
            other = lax.rem(me + d, n)
            pltpu.make_async_remote_copy(
                src_ref=src, dst_ref=dst.at[other], send_sem=send_sems.at[d - 1], recv_sem=recv_sems.at[other],
                device_id={axis: other}, device_id_type=MESH,
            ).wait_recv()
        for copy in copies:
            copy.wait_send()
        total = [dst[i] for i in range(n)]
        while len(total) > 1:
            total = [sum(total[i + 1 : i + 2], total[i]) for i in range(0, len(total), 2)]
        return total[0], done

    def phases():
        both = jnp.concatenate([bins_ref[...], bins_ref[...]], 1)
        turn = (both * pick_rows(starts, (SUB, 2 * n_bins))) & (NFFT - 1)
        turn = jnp.where(turn >= NFFT // 2, turn - NFFT, turn)
        angle = turn.astype(jnp.float32) * (2.0 * math.pi / NFFT)
        return jnp.cos(angle), jnp.sin(angle)

    part, _ = exchange("pts", pt, n_pts, gsend1, grecv1, s1, r1)
    gsend2[...] = part
    grecv2[fr] = part
    gram, (ph_re, ph_im) = exchange("freq", fr, n_freq, gsend2, grecv2, s2, r2, phases)
    gram = gram * (1.0 / count)
    swapped = pltpu.roll(gram, n_bins, 1)
    entries = [(swapped if e % 2 else gram)[e // 2 : e // 2 + 1, :] for e in range(n_entries)]
    g_re = {(b, b): entries[b] for b in range(n_blocks)}
    g_im = {}
    for i, (a, c) in enumerate(pairs):
        g_re[a, c] = g_re[c, a] = entries[n_blocks + 2 * i]
        g_im[a, c] = entries[n_blocks + 2 * i + 1]
        g_im[c, a] = -g_im[a, c]

    def apply_gram(xr, xi):
        ur, ui = [], []
        for a in range(n_blocks):
            others = [c for c in range(n_blocks) if c != a]
            ur.append(
                sum([g_re[a, c] * xr[c] - g_im[a, c] * xi[c] for c in others], g_re[a, a] * xr[a])
            )
            ui.append(
                sum([g_re[a, c] * xi[c] + g_im[a, c] * xr[c] for c in others], g_re[a, a] * xi[a])
            )
        return ur, ui

    xr = [ph_re[b : b + 1, :] for b in range(n_blocks)]
    xi = [ph_im[b : b + 1, :] for b in range(n_blocks)]
    for _ in range(ITERS):
        ur, ui = apply_gram(xr, xi)
        squares = [r * r + i * i for r, i in zip(ur, ui)]
        inv = lax.rsqrt(sum(squares[1:], squares[0]))
        xr = [r * inv for r in ur]
        xi = [i * inv for i in ui]
    ur, ui = apply_gram(xr, xi)
    terms = [xr[b] * ur[b] + xi[b] * ui[b] for b in range(n_blocks)]
    energy = sum(terms[1:], terms[0])
    chosen = jnp.zeros((1, per), jnp.float32)
    for f in range(n_freq):
        chosen = jnp.where(fr == f, energy[:, f * per : (f + 1) * per], chosen)
    energy_ref[...] = chosen
    factor = lax.rsqrt(jnp.maximum(energy, 0.25))
    coef[...] = jnp.transpose(pick_rows([r * factor for r in xr + xi], (SUB, 2 * n_bins)))

    groups = n_bins // SUB
    per_group = SUB // per
    half = groups // 2
    my_group = fr // per_group
    order = [
        (1 - my_group // half) * half + lax.rem(lax.rem(my_group, half) + i, half) for i in range(half)
    ] + [(my_group // half) * half + lax.rem(lax.rem(my_group, half) + i, half) for i in range(1, half)]
    order.append(my_group)
    sent = []

    def ship(slot, place, dest):
        copy = pltpu.make_async_remote_copy(
            src_ref=laid.at[pl.ds(slot * SUB + place * per, per)],
            dst_ref=recv_ref.at[:, :, :, pl.ds(pl.multiple_of(fr * n_local, LANES), n_local)],
            send_sem=s3.at[len(sent)],
            recv_sem=r3.at[fr],
            device_id={"freq": dest},
            device_id_type=MESH,
        )
        copy.start()
        sent.append(copy)

    for slot, g in enumerate(order):
        first = pl.multiple_of(g * SUB, SUB)
        col = coef[pl.ds(first, SUB), :]
        cr = [jnp.broadcast_to(col[:, b : b + 1], (SUB, LANES)) for b in range(n_blocks)]
        ci = [
            jnp.broadcast_to(col[:, n_blocks + b : n_blocks + b + 1], (SUB, LANES)) for b in range(n_blocks)
        ]
        for j in range(n_var * tiles):
            lane = slice(j * LANES, (j + 1) * LANES)
            re = im = None
            for b in range(n_blocks):
                sr = spec[pl.ds(pl.multiple_of(b * 2 * n_bins + first, SUB), SUB), lane]
                si = spec[pl.ds(pl.multiple_of((b * 2 + 1) * n_bins + first, SUB), SUB), lane]
                tr = cr[b] * sr - ci[b] * si
                ti = cr[b] * si + ci[b] * sr
                re = tr if re is None else re + tr
                im = ti if im is None else im + ti
            send[pl.ds(slot * SUB * step + j * 2, SUB, stride=step), :] = re
            send[pl.ds(slot * SUB * step + j * 2 + 1, SUB, stride=step), :] = im
        for k in range(slot * SUB, (slot + 1) * SUB):
            for v in range(n_var):
                for l in range(tiles):
                    row = k * step + (v * tiles + l) * 2
                    laid[k, v, :, l * LANES : (l + 1) * LANES] = send[row : row + 2, :]
        if slot < groups - 1:
            for place in range(per_group):
                ship(slot, place, g * per_group + place)
        else:
            here = lax.rem(fr, per_group)
            for r in range(1, per_group):
                place = lax.rem(here + r, per_group)
                ship(slot, place, g * per_group + place)
            own = pltpu.make_async_copy(
                laid.at[pl.ds(slot * SUB + here * per, per)],
                recv_ref.at[:, :, :, pl.ds(pl.multiple_of(fr * n_local, LANES), n_local)],
                own_sem,
            )
            own.start()
    for copy in sent:
        copy.wait_send()
    own.wait()
    for d in range(1, n_freq):
        other = lax.rem(fr + d, n_freq)
        pltpu.make_async_remote_copy(
            src_ref=laid.at[pl.ds(0, per)],
            dst_ref=recv_ref.at[:, :, :, pl.ds(pl.multiple_of(other * n_local, LANES), n_local)],
            send_sem=s3.at[0], recv_sem=r3.at[other], device_id={"freq": other}, device_id_type=MESH,
        ).wait_recv()


def place(recv, energy, out_hbm, mine_hbm, out_sem):
    per = recv.shape[0]
    stores = [pltpu.make_async_copy(energy, mine_hbm, out_sem.at[per])]
    stores += [pltpu.make_async_copy(recv.at[k], out_hbm.at[k], out_sem.at[k]) for k in range(per)]
    for copy in stores:
        copy.start()
    for copy in stores:
        copy.wait()


def body(n_freq, n_pts, snapshots, weights, starts, bins):
    n_time, n_var, n_local = snapshots.shape
    n_blocks = starts.shape[0]
    n_bins = bins.shape[0]
    per = n_bins // n_freq
    tiles = n_local // LANES
    step = n_var * tiles * 2
    count = float(n_local * n_freq * n_pts * n_var)
    f32 = jnp.float32
    entries = n_blocks * n_blocks + (n_blocks * n_blocks) % 2
    vmem = pl.BlockSpec(memory_space=pltpu.VMEM)
    anyspace = pl.BlockSpec(memory_space=pl.ANY)
    dma = pltpu.SemaphoreType.DMA
    recv, energy = pl.pallas_call(
        functools.partial(kernel, n_freq, n_pts, n_blocks, count),
        out_shape=(
            pltpu.VMEM((per, n_var, 2, n_freq * n_local), f32),
            pltpu.VMEM((1, per), f32),
        ),
        in_specs=[anyspace] * 7,
        out_specs=(vmem, vmem),
        scratch_shapes=[
            pltpu.VMEM((n_var, n_time, n_local), f32),
            pltpu.VMEM((1, n_local), f32),
            pltpu.VMEM((1, n_bins), jnp.int32),
            pltpu.VMEM((NFFT // 2, 2 * NFFT), f32),
            pltpu.VMEM((n_time - NFFT + 1, n_time), f32),
            pltpu.VMEM((n_bins, 2 * NFFT), f32),
            pltpu.VMEM((n_blocks * 2 * n_bins, 3 * n_time), jnp.bfloat16),
            pltpu.VMEM((n_blocks * 2 * n_bins, n_var * n_local), f32),
            pltpu.VMEM((entries * n_bins, LANES), f32),
            pltpu.VMEM((entries // 2, 2 * n_bins), f32),
            pltpu.VMEM((n_pts, entries // 2, 2 * n_bins), f32),
            pltpu.VMEM((entries // 2, 2 * n_bins), f32),
            pltpu.VMEM((n_freq, entries // 2, 2 * n_bins), f32),
            pltpu.VMEM((2 * n_bins, SUB), f32),
            pltpu.VMEM((n_bins * step, LANES), f32),
            pltpu.VMEM((n_bins, n_var, 2, n_local), f32),
            pltpu.SMEM((n_blocks,), jnp.int32),
            pltpu.SMEM((n_bins,), jnp.int32),
            dma((n_var,)),
            dma((6,)),
            dma((n_pts,)),
            dma((n_pts,)),
            dma((n_freq,)),
            dma((n_freq,)),
            dma((n_freq,)),
            dma((n_freq,)),
            dma,
        ],
        compiler_params=pltpu.CompilerParams(collective_id=0, has_side_effects=True),
    )(
        jnp.transpose(snapshots, (1, 0, 2)), weights.reshape(1, n_local), starts, bins,
        bins.reshape(1, n_bins), jnp.asarray(base_table(NFFT)), jnp.asarray(window_table(NFFT, n_time)),
    )
    modes, mine = pl.pallas_call(
        place,
        out_shape=(
            jax.ShapeDtypeStruct((per, n_var, 2, n_freq * n_local), f32),
            jax.ShapeDtypeStruct((1, per), f32),
        ),
        in_specs=[vmem, vmem],
        out_specs=(anyspace, anyspace),
        scratch_shapes=[dma((per + 1,))],
    )(pltpu.with_memory_space_constraint(recv, pltpu.VMEM), pltpu.with_memory_space_constraint(energy, pltpu.VMEM))
    return jnp.transpose(modes, (0, 2, 1, 3)), mine[0]


def solution(mesh):
    in_specs = (P(None, None, ("pts", "freq")), P(("pts", "freq")), P(), P())
    out_specs = (P("freq", None, None, "pts"), P("freq"))
    f = functools.partial(body, mesh.shape["freq"], mesh.shape["pts"])
    return jax.shard_map(f, mesh=mesh, in_specs=in_specs, out_specs=out_specs, check_vma=False)
```
